32 devices in a mesh: comp: 2 (over x), gy: 4 (over z), gx: 4 (over y, core).
Axes of the slice: x: 2, y: 2, z: 4, core: 2. Of those that a mesh axis runs over, the one named last changes fastest.
Arguments:
- column_water: float32 [2, 16, 32, 512], P('comp', None, 'gy', 'gx'), may hold values from 0.2 to 2
- land_soil: float32 [2, 32, 512], P('comp', 'gy', 'gx'), may hold values from 0.1 to 0.9
- level_weight: float32 [16], replicated, may hold values from 0.01 to 0.1
- excess_weight: float32 [16], replicated, may hold values from 0.3 to 3
- soil_weight: float32 [16], replicated, may hold values from 0.3 to 3
- terrain_class: int32 [320, 5120], P('gy', 'gx'), may hold values from 0 to 15
- surface_head: float32 [2, 320, 5120], P('comp', 'gy', 'gx'), may hold values from 0 to 1
- conductivity: float32 [2, 320, 5120], P('comp', 'gy', 'gx'), may hold values from 0.02 to 0.22
- active_mask: int32 [2, 320, 5120], P('comp', 'gy', 'gx'), may hold values 0 or 1
- flow_code: int32 [2, 320, 5120], P('comp', 'gy', 'gx'), may hold values from 0 to 3
Outputs:
- coupled_state: float32 [2, 32, 512], P('comp', 'gy', 'gx')
The draws below stay inside these ranges and needn't reach their ends.
All inputs are finite; a program needn't handle non-finite values. No bound on the sum of `active_mask` on one device may be relied on, other than what follows from the above.
Results may differ from the reference program's by a relative error of at most 0.0003.
Values sent between devices are 32-bit elements; how exact they have to be, the bound alone decides.
A program may use at most 64 MiB of HBM per device.

```python
import math
import jax
import jax.numpy as jnp
from jax import lax

LEV = 16
AGG = 10
NW = 16
NSUB = 8
SWEEPS = 2
NYC = 32
NXC = 512
NYF = 320
NXF = 5120


def with_ends(values, stream_key, smallest, largest):
    dims = values.shape
    place = [jax.random.randint(jax.random.fold_in(stream_key, axis), (), 0, dims[axis]) for axis in range(len(dims))]
    values = values.at[tuple(place)].set(smallest)
    longest = dims.index(max(dims))
    place[longest] = (place[longest] + 1) % dims[longest]
    return values.at[tuple(place)].set(largest)


def levels(stream_key, extent, shards, smallest, high):
    gain, own = 1.0, jax.random.fold_in(stream_key, 6)
    for axis_at, parts in shards:
        steps = jnp.exp(jax.random.uniform(jax.random.fold_in(own, axis_at), (parts,), jnp.float32, smallest / len(shards), high / len(shards)))
        gain = gain * jnp.repeat(steps, extent[axis_at] // parts).reshape([-1 if axis == axis_at else 1 for axis in range(len(extent))])
    return gain


def setup_inputs(seed: int = 0) -> dict:
    key_list = jax.random.split(jax.random.key(seed), 11)
    return {
        "column_water": jnp.clip(jnp.exp(math.log(2.0) - 2.3025851 * jax.random.uniform(key_list[0], (2, LEV, NYC, NXC), jnp.float32) ** levels(key_list[0], (2, LEV, NYC, NXC), ((0, 2), (2, 4), (3, 4)), -0.2, 0.2)), 0.2, 2.0),
        "land_soil": jnp.clip(0.1 + 0.79999997 * jax.random.uniform(key_list[1], (2, NYC, NXC), jnp.float32) ** levels(key_list[1], (2, NYC, NXC), ((0, 2), (1, 4), (2, 4)), -0.2, 0.2), 0.1, 0.9),
        "level_weight": jnp.clip(jnp.exp(jax.random.uniform(key_list[2], (LEV,), jnp.float32, math.log(0.01), math.log(0.1))), 0.01, 0.1),
        "excess_weight": jnp.clip(jnp.exp(jax.random.uniform(key_list[3], (NW,), jnp.float32, math.log(0.3), math.log(3.0))), 0.3, 3.0),
        "soil_weight": jnp.clip(jnp.exp(jax.random.uniform(key_list[4], (NW,), jnp.float32, math.log(0.3), math.log(3.0))), 0.3, 3.0),
        "terrain_class": with_ends(jax.random.randint(key_list[5], (NYF, NXF), 0, NW), jax.random.fold_in(key_list[5], 1), 0, NW - 1).astype(jnp.int32),
        "surface_head": jnp.clip(1.0 * jax.random.uniform(key_list[6], (2, NYF, NXF), jnp.float32) ** levels(key_list[6], (2, NYF, NXF), ((0, 2), (1, 4), (2, 4)), -0.2, 0.2), 0.0, 1.0),
        "conductivity": jnp.clip(jnp.exp(math.log(0.22) - 2.3978953 * jax.random.uniform(key_list[7], (2, NYF, NXF), jnp.float32) ** levels(key_list[7], (2, NYF, NXF), ((0, 2), (1, 4), (2, 4)), -0.2, 0.2)), 0.02, 0.22),
        "active_mask": with_ends((jax.random.randint(key_list[8], (2, NYF, NXF), 0, 10) < 9).astype(jnp.int32), jax.random.fold_in(key_list[8], 1), 0, 1),
        "flow_code": with_ends(jax.random.randint(key_list[9], (2, NYF, NXF), 0, 4), jax.random.fold_in(key_list[9], 1), 0, 3).astype(jnp.int32),
    }


diffusion_rate = 0.2
infiltration_rate = 0.05
drainage_rate = 0.1
half_point = 0.1
evaporation_scale = 0.5

def neighbours(field):
    return (field[:-2, 1:-1], field[2:, 1:-1], field[1:-1, :-2], field[1:-1, 2:])

def lookup(table, classes):
    summed = jnp.zeros(classes.shape, table.dtype)
    for number in range(table.shape[0]):
        summed = summed + jnp.where(classes == number, table[number], 0.0)
    return summed

def block_mean(field):
    rows, cols = field.shape
    return field.reshape(rows // AGG, AGG, cols // AGG, AGG).mean(axis=(1, 3))

def upsample(field):
    return jnp.repeat(jnp.repeat(field, AGG, axis=0), AGG, axis=1)

def disaggregate(coarse, weights):
    return upsample(coarse) * (weights / upsample(block_mean(weights)))

def smooth(padded, field):
    beside_all = padded[:, :-2, 1:-1] + padded[:, 2:, 1:-1] + padded[:, 1:-1, :-2] + padded[:, 1:-1, 2:]
    return field + diffusion_rate * (beside_all - 4.0 * field)

def route_step(water, moisture, keff, active, codes):
    drained = drainage_rate * active * moisture * moisture
    centre_keff = keff[1:-1, 1:-1]
    centre_water = water[1:-1, 1:-1]
    centre_moist = moisture[1:-1, 1:-1]
    spread = jnp.zeros_like(centre_water)
    for keff_side, water_side in zip(neighbours(keff), neighbours(water)):
        spread = spread + jnp.sqrt(centre_keff * keff_side) * (water_side - centre_water)
    northern, southern, western, eastern = neighbours(drained)
    code_north, code_south, code_west, code_east = neighbours(codes)
    inflow = jnp.where(code_south == 0, southern, 0.0) + jnp.where(code_north == 1, northern, 0.0)
    inflow = inflow + jnp.where(code_east == 2, eastern, 0.0) + jnp.where(code_west == 3, western, 0.0)
    soaked = infiltration_rate * centre_water / (1.0 + centre_moist)
    return (centre_water + spread - soaked, centre_moist + soaked - drained[1:-1, 1:-1] + inflow)

def reference(column_water, land_soil, level_weight, excess_weight, soil_weight, terrain_class, surface_head, conductivity, active_mask, flow_code):
    water = column_water[0]
    for counter in range(SWEEPS):
        water = smooth(jnp.pad(water, ((0, 0), (1, 1), (1, 1))), water)
    precip = lax.optimization_barrier(jnp.sum(level_weight[:, None, None] * water * water, axis=0))
    moisture = land_soil[0]
    excess = precip * moisture * moisture / (moisture * moisture + half_point)
    excess_fine = disaggregate(excess, lookup(excess_weight, terrain_class))
    soil_fine = disaggregate(moisture, lookup(soil_weight, terrain_class))
    active = active_mask[1].astype(jnp.float32)
    keff = conductivity[1] * active
    codes = flow_code[1]
    ponded = active * (surface_head[1] + excess_fine)
    stored = soil_fine
    for counter in range(NSUB):
        ponded, stored = route_step(jnp.pad(ponded, 1), jnp.pad(stored, 1), jnp.pad(keff, 1), jnp.pad(active, 1), jnp.pad(codes, 1))
    land_out = block_mean(stored) / (1.0 + evaporation_scale * water[0] * water[0])
    return jnp.stack([land_out, block_mean(ponded)])
```

```python
import functools

import jax
import jax.numpy as jnp
from jax import lax
from jax.experimental import pallas as pl
from jax.experimental.pallas import tpu as pltpu
from jax.sharding import PartitionSpec as P

AGG = 10
NSUB = 8
SWEEPS = 2

diffusion_rate = 0.2
infiltration_rate = 0.05
drainage_rate = 0.1
half_point = 0.1
evaporation_scale = 0.5

LANE = 128
SUB = 8
MESH = pl.DeviceIdType.MESH
DIRS = ((-1, 0), (1, 0), (0, -1), (0, 1), (-1, -1), (-1, 1), (1, -1), (1, 1))
N, S, W, E, NW, NE, SW, SE = range(8)
OPP = (S, N, E, W, SE, SW, NE, NW)


def iota(shape, dim):
    return lax.broadcasted_iota(jnp.int32, shape, dim)


def pick(table, classes):
    values = [table[k] for k in range(table.shape[0])]
    bit = 1
    while len(values) > 1:
        odd = (classes & bit) != 0
        values = [
            jnp.where(odd, values[k + 1], values[k]) for k in range(0, len(values), 2)
        ]
        bit *= 2
    return values[0]


def halves(x):
    high = x.astype(jnp.bfloat16)
    return high, (x - high.astype(jnp.float32)).astype(jnp.bfloat16)


def kernel(
    ny, nx,
    lw, ewt, swt, water_in, soil_in, terrain_in, head_in, cond_in, active_in, code_in,
    out_ref,
    xi, xf, st, ps, wb, mb, pk, dg, mn, qb, qx, back_tx, back_rx, gather, spreadm,
    send, recv, local, hop,
):
    group = lax.axis_index("comp")
    gy = lax.axis_index("gy")
    gx = lax.axis_index("gx")
    rows, cols = terrain_in.shape
    lev = water_in.shape[1]
    crow, ccol = soil_in.shape[1], soil_in.shape[2]
    tiles = cols // LANE
    width = tiles + 1
    bands = rows // SUB + 2

    lane = iota((SUB, LANE), 1)
    sub = iota((SUB, LANE), 0)

    def exists(d):
        dy, dx = DIRS[d]
        return (gy + dy >= 0) & (gy + dy < ny) & (gx + dx >= 0) & (gx + dx < nx)

    def at(d):
        dy, dx = DIRS[d]
        return {"comp": group, "gy": gy + dy, "gx": gx + dx}

    partner = {"comp": 1 - group, "gy": gy, "gx": gx}

    def copy(src, dst, d, f):
        return pltpu.make_async_remote_copy(
            src_ref=src, dst_ref=dst, send_sem=send.at[d, f], recv_sem=recv.at[OPP[d], f],
            device_id=at(d), device_id_type=MESH,
        )

    def arrival(dst, d, f):
        return pltpu.make_async_remote_copy(
            src_ref=dst, dst_ref=dst, send_sem=send.at[d, f], recv_sem=recv.at[d, f],
            device_id=at(d), device_id_type=MESH,
        )

    fields = (
        (cond_in.at[0], xf.at[0]),
        (active_in.at[0], xi.at[1]),
        (code_in.at[0], xi.at[2]),
        (head_in.at[0], xf.at[1]),
        (terrain_in, xi.at[0]),
    )
    rfrom = {-1: (0, SUB), 0: (0, rows), 1: (rows - SUB, SUB)}
    cfrom = {-1: (0, LANE), 0: (0, cols), 1: (cols - LANE, LANE)}
    rslot = {-1: (0, SUB), 0: (SUB, rows), 1: (rows + SUB, SUB)}
    cslot = {-1: (cols + LANE, LANE), 0: (0, cols), 1: (cols, LANE)}

    def cut(ref, r, c):
        return ref.at[pl.ds(r[0], r[1]), pl.ds(c[0], c[1])]

    def part(ref, d):
        return cut(ref, rfrom[DIRS[d][0]], cfrom[DIRS[d][1]])

    def slot(ref, d):
        return cut(ref, rslot[DIRS[d][0]], cslot[DIRS[d][1]])

    own = ((SUB, rows), (0, cols))

    def local_copy(src, dst, k):
        return pltpu.make_async_copy(src, dst, local.at[k])

    terrain_load = local_copy(terrain_in, cut(xi.at[0], *own), 4)
    route_loads = [local_copy(f[0], cut(f[1], *own), k) for k, f in enumerate(fields[:4])]
    water_load = local_copy(water_in.at[0], wb.at[8], 0)
    soil_load = local_copy(soil_in.at[0], mb.at[8], 1)

    barrier = pltpu.get_barrier_semaphore()
    for d in range(8):
        @pl.when(exists(d))
        def _():
            pl.semaphore_signal(barrier, inc=1, device_id=at(d), device_id_type=MESH)
    pl.semaphore_signal(barrier, inc=1, device_id=partner, device_id_type=MESH)
    greeted = 1
    for d in range(8):
        greeted = greeted + exists(d).astype(jnp.int32)

    terrain_load.start()

    @pl.when(group == 0)
    def _():
        water_load.start()
        soil_load.start()

    @pl.when(group == 1)
    def _():
        for load in route_loads:
            load.start()

    pl.semaphore_wait(barrier, greeted)

    def land_first(d):
        out = [copy(soil_in.at[0], mb.at[OPP[d]], d, 1)]
        if d < 4:
            out.insert(0, copy(water_in.at[0], wb.at[OPP[d]], d, 0))
        return out

    def land_pack(d):
        return copy(pk.at[0 if DIRS[d][1] < 0 else 1], dg.at[OPP[d] - 4], d, 0)

    def land_mean(d):
        return copy(mn.at[8], mn.at[OPP[d]], d, 2)

    def route_sends(d):
        return [copy(part(f[0], d), slot(f[1], OPP[d]), d, k) for k, f in enumerate(fields)]

    q_send = pltpu.make_async_remote_copy(
        src_ref=qb.at[0], dst_ref=qb.at[1], send_sem=hop.at[0], recv_sem=hop.at[1],
        device_id=partner, device_id_type=MESH,
    )
    back_send = pltpu.make_async_remote_copy(
        src_ref=back_tx, dst_ref=back_rx, send_sem=hop.at[2], recv_sem=hop.at[3],
        device_id=partner, device_id_type=MESH,
    )

    def over(dirs, act):
        for d in dirs:
            @pl.when(exists(d))
            def _():
                act(d)

    def start_all(copies):
        for c in copies:
            c.start()

    @pl.when(group == 0)
    def _():
        over(range(8), lambda d: start_all(land_first(d)))

    @pl.when(group == 1)
    def _():
        over(range(8), lambda d: start_all(route_sends(d)))

    k10 = iota((LANE, ccol), 1) * AGG
    j0 = iota((LANE, ccol), 0)

    for c in range(tiles):
        j = j0 + c * LANE
        gather[c * LANE : (c + 1) * LANE, :] = jnp.where(
            (j >= k10) & (j < k10 + AGG), 1.0, 0.0
        ).astype(jnp.bfloat16)

    def means(first, second):
        parts = []
        for field in (first, second):
            high, low = [], []
            for tile in field:
                a, b = halves(tile)
                high.append(a)
                low.append(b)
            parts.append(jnp.concatenate(high, axis=1))
            parts.append(jnp.concatenate(low, axis=1))
        stacked = jnp.concatenate(parts, axis=0)
        y = jnp.dot(stacked, gather[...], preferred_element_type=jnp.float32)
        i10 = iota((crow, rows), 0) * AGG
        i = iota((crow, rows), 1)
        pool = jnp.where((i >= i10) & (i < i10 + AGG), 1.0, 0.0)
        total = []
        for k in (0, 2):
            z = y[k * rows : (k + 1) * rows] + y[(k + 1) * rows : (k + 2) * rows]
            total.append(
                jnp.dot(pool, z, preferred_element_type=jnp.float32, precision=lax.Precision.HIGHEST)
                * (1.0 / (AGG * AGG))
            )
        return total

    @pl.when(group == 0)
    def _():
        water_load.wait()
        packs = [jnp.zeros((SUB, LANE), jnp.float32), jnp.zeros((SUB, LANE), jnp.float32)]
        for l in range(lev):
            mine = (lane >= 8 * l) & (lane < 8 * l + 8)
            w = wb[8, l]
            packs[0] = jnp.where(mine, pltpu.roll(w, (8 * l) % LANE, 1), packs[0])
            packs[1] = jnp.where(mine, pltpu.roll(w, (8 * l + 8) % LANE, 1), packs[1])
        pk[0] = packs[0]
        pk[1] = packs[1]
        over(range(4, 8), lambda d: land_pack(d).start())

        terrain_load.wait()
        firsts, seconds = [], []
        for c in range(tiles):
            tc = xi[0, SUB : SUB + rows, c * LANE : (c + 1) * LANE]
            firsts.append(pick(ewt, tc))
            seconds.append(pick(swt, tc))
        mean_e, mean_s = means(firsts, seconds)
        mn[8, 0] = mean_e
        mn[8, 1] = mean_s
        over(range(8), lambda d: land_mean(d).start())

        soil_load.wait()
        over(range(4), lambda d: arrival(wb.at[d], d, 0).wait_recv())
        over(range(4, 8), lambda d: arrival(dg.at[d - 4], d, 0).wait_recv())
        over(range(8), lambda d: arrival(mb.at[d], d, 1).wait_recv())

        def valid(a, b):
            r = sub + (0 if a == 0 else jnp.where(sub < 4, crow, -crow))
            r = r + gy * crow
            k = lane + (0 if b == 0 else jnp.where(lane < 64, ccol, -ccol))
            k = k + gx * ccol
            return (r >= 0) & (r < ny * crow) & (k >= 0) & (k < nx * ccol)

        ok = [[valid(a, b) for b in range(2)] for a in range(2)]
        left = lane < 64
        upper = sub < 4

        def joined(get, corner, fill):
            t = [
                [get(8), jnp.where(left, get(E), get(W))],
                [jnp.where(upper, get(S), get(N)), corner],
            ]
            return [[jnp.where(ok[a][b], t[a][b], fill) for b in range(2)] for a in range(2)]

        def corners(get):
            return jnp.where(
                upper,
                jnp.where(left, get(SE), get(SW)),
                jnp.where(left, get(NE), get(NW)),
            )

        def smooth(t):
            new = [[None, None], [None, None]]
            down = [[pltpu.roll(t[a][b], 1, 0) for b in range(2)] for a in range(2)]
            up = [[pltpu.roll(t[a][b], SUB - 1, 0) for b in range(2)] for a in range(2)]
            right = [[pltpu.roll(t[a][b], 1, 1) for b in range(2)] for a in range(2)]
            lft = [[pltpu.roll(t[a][b], LANE - 1, 1) for b in range(2)] for a in range(2)]
            for a in range(2):
                for b in range(2):
                    around = (
                        jnp.where(sub == 0, down[1 - a][b], down[a][b])
                        + jnp.where(sub == SUB - 1, up[1 - a][b], up[a][b])
                        + jnp.where(lane == 0, right[a][1 - b], right[a][b])
                        + jnp.where(lane == LANE - 1, lft[a][1 - b], lft[a][b])
                    )
                    value = t[a][b] + diffusion_rate * (around - 4.0 * t[a][b])
                    new[a][b] = jnp.where(ok[a][b], value, 0.0)
            return new

        ce = jnp.where(upper, dg[SE - 4], dg[NE - 4])
        cw = jnp.where(upper, dg[SW - 4], dg[NW - 4])
        precip = [[0.0, 0.0], [0.0, 0.0]]
        ground = None
        for l in range(lev):
            corner = jnp.where(
                left,
                pltpu.roll(ce, (LANE - 8 * l) % LANE, 1),
                pltpu.roll(cw, (2 * LANE - 8 - 8 * l) % LANE, 1),
            )
            t = joined(lambda k: wb[k, l], corner, 0.0)
            for _ in range(SWEEPS):
                t = smooth(t)
            if l == 0:
                ground = t[0][0]
            for a in range(2):
                for b in range(2):
                    precip[a][b] = precip[a][b] + lw[l] * t[a][b] * t[a][b]

        moisture = joined(lambda k: mb[k], corners(lambda k: mb[k]), 0.5)
        over(range(8), lambda d: arrival(mn.at[d], d, 2).wait_recv())
        m_e = joined(lambda k: mn[k, 0], corners(lambda k: mn[k, 0]), 1.0)
        m_s = joined(lambda k: mn[k, 1], corners(lambda k: mn[k, 1]), 1.0)
        for a in range(2):
            for b in range(2):
                m = moisture[a][b]
                excess = precip[a][b] * m * m / (m * m + half_point)
                rs = slice(a * SUB, (a + 1) * SUB)
                cs = slice(b * LANE, (b + 1) * LANE)
                qb[0, 0, rs, cs] = excess / m_e[a][b]
                qb[0, 1, rs, cs] = m / m_s[a][b]
        q_send.start()
        divisor = 1.0 + evaporation_scale * ground * ground
        over(range(8), lambda d: [c.wait_send() for c in land_first(d)])
        over(range(4, 8), lambda d: land_pack(d).wait_send())
        over(range(8), lambda d: land_mean(d).wait_send())
        q_send.wait_send()
        back_send.wait_recv()
        out_ref[0] = back_rx[...] / divisor

    R, AD, M0, M1, M2, M3, EW, HD, SO = range(9)
    WN, WS, WW, WE, AA, B0, B1, B2, B3 = range(9, 18)

    @pl.when(group == 1)
    def _():
        kk = iota((2 * ccol, LANE), 0)
        jj = iota((2 * ccol, LANE), 1)
        for c in range(tiles):
            j = jj + c * LANE
            spreadm[:, c * LANE : (c + 1) * LANE] = jnp.where(
                (j >= kk * AGG) & (j < kk * AGG + AGG), 1.0, 0.0
            ).astype(jnp.bfloat16)
        spreadm[:, cols:] = jnp.where(
            ((jj < 64) & (kk == ccol)) | ((jj >= 64) & (kk == 2 * ccol - 1)), 1.0, 0.0
        ).astype(jnp.bfloat16)

        zero = jnp.zeros((SUB, LANE), jnp.float32)
        for c in range(width):
            for edge in (0, (bands + 1) * SUB):
                for k in (R, M0, M1):
                    st[k, c, edge : edge + SUB] = zero
                for k in range(2):
                    for p in range(2):
                        ps[p, k, c, edge : edge + SUB] = zero

        def prepare(t, c):
            r = pl.ds(t * SUB if isinstance(t, int) else pl.multiple_of(t * SUB, SUB), SUB)
            o = pl.ds(
                (t + 1) * SUB if isinstance(t, int) else pl.multiple_of(t * SUB + SUB, SUB), SUB
            )

            def take(ref, k):
                a = ref[k, r, c * LANE : (c + 1) * LANE]
                if c < tiles:
                    return a
                return jnp.where(lane < 64, a, ref[k, r, (c + 1) * LANE : (c + 2) * LANE])

            row = sub + (t - 1) * SUB + gy * rows
            col = lane + c * LANE
            if c == tiles:
                col = jnp.where(lane < 64, col, lane - LANE)
            col = col + gx * cols
            ok = (row >= 0) & (row < ny * rows) & (col >= 0) & (col < nx * cols)
            active = jnp.where(ok, take(xi, 1).astype(jnp.float32), 0.0)
            code = take(xi, 2)
            keff = jnp.where(ok, take(xf, 0), 0.0) * active
            tc = take(xi, 0)
            st[R, c, o] = jnp.sqrt(keff)
            rate = drainage_rate * active
            st[AD, c, o] = rate
            for k in range(4):
                st[M0 + k, c, o] = jnp.where(code == k, rate, 0.0)
            st[EW, c, o] = active * pick(ewt, tc)
            st[HD, c, o] = active * jnp.where(ok, take(xf, 1), 0.0)
            st[SO, c, o] = pick(swt, tc)

        for load in route_loads:
            load.wait()
        terrain_load.wait()

        def inner(t, carry):
            for c in range(tiles):
                prepare(t, c)
            return carry

        lax.fori_loop(1, bands - 1, inner, 0)

        over(range(8), lambda d: [arrival(slot(f[1], d), d, k).wait_recv() for k, f in enumerate(fields)])

        def rim(k, carry):
            for c in range(tiles):
                prepare(k * (bands - 1), c)
            return carry

        lax.fori_loop(0, 2, rim, 0)

        def side(t, carry):
            prepare(t, tiles)
            return carry

        lax.fori_loop(0, bands, side, 0)

        def from_west(tile_list):
            turned = [pltpu.roll(x, 1, 1) for x in tile_list]
            return [jnp.where(lane == 0, turned[c - 1], turned[c]) for c in range(width)]

        def from_east(tile_list):
            turned = [pltpu.roll(x, LANE - 1, 1) for x in tile_list]
            return [
                jnp.where(lane == LANE - 1, turned[(c + 1) % width], turned[c])
                for c in range(width)
            ]

        def couple(t, carry):
            base = pl.multiple_of(t * SUB + SUB, SUB)
            o = pl.ds(base, SUB)
            above = pl.ds(base - 1, SUB)
            below = pl.ds(base + 1, SUB)
            r = [st[R, c, o] for c in range(width)]
            west, east = from_west(r), from_east(r)
            for c in range(width):
                wn = r[c] * st[R, c, above]
                ws = r[c] * st[R, c, below]
                ww = r[c] * west[c]
                we = r[c] * east[c]
                st[WN, c, o] = wn
                st[WS, c, o] = ws
                st[WW, c, o] = ww
                st[WE, c, o] = we
                st[AA, c, o] = (wn + ws) + (ww + we)
                st[B0, c, o] = st[M0, c, below]
                st[B1, c, o] = st[M1, c, above]
            for c, v in enumerate(from_east([st[M2, c, o] for c in range(width)])):
                st[B2, c, o] = v
            for c, v in enumerate(from_west([st[M3, c, o] for c in range(width)])):
                st[B3, c, o] = v
            return carry

        lax.fori_loop(0, bands, couple, 0)

        q_send.wait_recv()
        high, low = [], []
        for k in range(2):
            a, b = halves(qb[1, k])
            high.append(a)
            low.append(b)
        y = jnp.dot(
            jnp.concatenate(high + low, axis=0), spreadm[...], preferred_element_type=jnp.float32
        )
        qx[...] = y[: 4 * SUB] + y[4 * SUB :]
        for t in range(bands):
            o = slice((t + 1) * SUB, (t + 2) * SUB)
            if t == 0:
                a = b = 2 * crow - 1
            elif t == bands - 1:
                a = b = crow
            else:
                a, b = ((t - 1) * SUB) // AGG, ((t - 1) * SUB + SUB - 1) // AGG
            for c in range(width):
                cs = slice(c * LANE, (c + 1) * LANE)

                def up(k):
                    first = jnp.broadcast_to(qx[k * 16 + a : k * 16 + a + 1, cs], (SUB, LANE))
                    if a == b:
                        return first
                    second = jnp.broadcast_to(qx[k * 16 + b : k * 16 + b + 1, cs], (SUB, LANE))
                    return jnp.where(sub < b * AGG - (t - 1) * SUB, first, second)

                ps[0, 0, c, o] = st[HD, c, o] + st[EW, c, o] * up(0)
                ps[0, 1, c, o] = st[SO, c, o] * up(1)

        def substep(src, dst):
            def band(t, carry):
                base = pl.multiple_of(t * SUB + SUB, SUB)
                o = pl.ds(base, SUB)
                above = pl.ds(base - 1, SUB)
                below = pl.ds(base + 1, SUB)
                p = [ps[src, 0, c, o] for c in range(width)]
                s = [ps[src, 1, c, o] for c in range(width)]
                ss = [x * x for x in s]
                p_w, p_e = from_west(p), from_east(p)
                s_w, s_e = from_west(ss), from_east(ss)
                for c in range(width):
                    s_n = ps[src, 1, c, above]
                    s_s = ps[src, 1, c, below]
                    spread = (
                        st[WN, c, o] * ps[src, 0, c, above]
                        + st[WS, c, o] * ps[src, 0, c, below]
                        + (st[WW, c, o] * p_w[c] + st[WE, c, o] * p_e[c])
                        - st[AA, c, o] * p[c]
                    )
                    soaked = infiltration_rate * p[c] * pl.reciprocal(1.0 + s[c])
                    inflow = (
                        st[B0, c, o] * (s_s * s_s)
                        + st[B1, c, o] * (s_n * s_n)
                        + (st[B2, c, o] * s_e[c] + st[B3, c, o] * s_w[c])
                        - st[AD, c, o] * ss[c]
                    )
                    ps[dst, 0, c, o] = p[c] + (spread - soaked)
                    ps[dst, 1, c, o] = s[c] + (soaked + inflow)
                return carry

            lax.fori_loop(0, bands, band, 0)

        def two(k, carry):
            substep(0, 1)
            substep(1, 0)
            return carry

        lax.fori_loop(0, NSUB // 2, two, 0)

        inside = slice(2 * SUB, 2 * SUB + rows)
        mean_p, mean_st = means(
            [ps[0, 0, c, inside] for c in range(tiles)],
            [ps[0, 1, c, inside] for c in range(tiles)],
        )
        back_tx[...] = mean_st
        back_send.start()
        out_ref[0] = mean_p
        over(range(8), lambda d: [c.wait_send() for c in route_sends(d)])
        back_send.wait_send()


def per_device(ny, nx, column_water, land_soil, level_weight, excess_weight, soil_weight,
               terrain_class, surface_head, conductivity, active_mask, flow_code):
    rows, cols = terrain_class.shape
    lev = column_water.shape[1]
    crow, ccol = land_soil.shape[1:]
    wide = cols // LANE + 1
    tall = rows + 4 * SUB
    f32, i32 = jnp.float32, jnp.int32
    any_spec = pl.BlockSpec(memory_space=pl.ANY)
    smem = pl.BlockSpec(memory_space=pltpu.SMEM)
    return pl.pallas_call(
        functools.partial(kernel, ny, nx),
        out_shape=jax.ShapeDtypeStruct((1, crow, ccol), f32),
        in_specs=[smem] * 3 + [any_spec] * 7,
        out_specs=pl.BlockSpec(memory_space=pltpu.VMEM),
        scratch_shapes=[
            pltpu.VMEM((3, rows + 2 * SUB, cols + 2 * LANE), i32),
            pltpu.VMEM((2, rows + 2 * SUB, cols + 2 * LANE), f32),
            pltpu.VMEM((18, wide, tall, LANE), f32),
            pltpu.VMEM((2, 2, wide, tall, LANE), f32),
            pltpu.VMEM((9, lev, crow, ccol), f32),
            pltpu.VMEM((9, crow, ccol), f32),
            pltpu.VMEM((2, crow, ccol), f32),
            pltpu.VMEM((4, crow, ccol), f32),
            pltpu.VMEM((9, 2, crow, ccol), f32),
            pltpu.VMEM((2, 2, 2 * crow, 2 * ccol), f32),
            pltpu.VMEM((4 * crow, cols + LANE), f32),
            pltpu.VMEM((crow, ccol), f32),
            pltpu.VMEM((crow, ccol), f32),
            pltpu.VMEM((cols, ccol), jnp.bfloat16),
            pltpu.VMEM((2 * ccol, cols + LANE), jnp.bfloat16),
            pltpu.SemaphoreType.DMA((8, 5)),
            pltpu.SemaphoreType.DMA((8, 5)),
            pltpu.SemaphoreType.DMA((5,)),
            pltpu.SemaphoreType.DMA((4,)),
        ],
        compiler_params=pltpu.CompilerParams(
            collective_id=0, has_side_effects=True, vmem_limit_bytes=48 * 1024 * 1024
        ),
    )(level_weight, excess_weight, soil_weight, column_water, land_soil, terrain_class,
      surface_head, conductivity, active_mask, flow_code)


def solution(mesh):
    in_specs = (
        P("comp", None, "gy", "gx"),
        P("comp", "gy", "gx"),
        P(),
        P(),
        P(),
        P("gy", "gx"),
        P("comp", "gy", "gx"),
        P("comp", "gy", "gx"),
        P("comp", "gy", "gx"),
        P("comp", "gy", "gx"),
    )
    body = functools.partial(per_device, mesh.shape["gy"], mesh.shape["gx"])
    return jax.shard_map(
        body, mesh=mesh, in_specs=in_specs, out_specs=P("comp", "gy", "gx"), check_vma=False
    )
```

```python
import functools

import jax
import jax.numpy as jnp
from jax import lax
from jax.experimental import pallas as pl
from jax.experimental.pallas import tpu as pltpu
from jax.sharding import PartitionSpec as P

AGG = 10
NSUB = 8
SWEEPS = 2

diffusion_rate = 0.2
infiltration_rate = 0.05
drainage_rate = 0.1
half_point = 0.1
evaporation_scale = 0.5

LANE = 128
SUB = 8
MESH = pl.DeviceIdType.MESH
DIRS = ((-1, 0), (1, 0), (0, -1), (0, 1), (-1, -1), (-1, 1), (1, -1), (1, 1))
N, S, W, E, NW, NE, SW, SE = range(8)
OPP = (S, N, E, W, SE, SW, NE, NW)


def iota(shape, dim):
    return lax.broadcasted_iota(jnp.int32, shape, dim)


def pick(table, classes):
    values = [table[k] for k in range(table.shape[0])]
    bit = 1
    while len(values) > 1:
        odd = (classes & bit) != 0
        values = [
            jnp.where(odd, values[k + 1], values[k]) for k in range(0, len(values), 2)
        ]
        bit *= 2
    return values[0]


def halves(x):
    high = x.astype(jnp.bfloat16)
    return high, (x - high.astype(jnp.float32)).astype(jnp.bfloat16)


def kernel(
    ny, nx,
    lw, ewt, swt, water_in, soil_in, terrain_in, head_in, cond_in, active_in, code_in,
    out_ref,
    xi, xf, st, ps, wb, mb, pk, dg, mn, qb, qx, back_tx, back_rx, gather, spreadm,
    send, recv, local, hop,
):
    group = lax.axis_index("comp")
    gy = lax.axis_index("gy")
    gx = lax.axis_index("gx")
    rows, cols = terrain_in.shape
    lev = water_in.shape[1]
    crow, ccol = soil_in.shape[1], soil_in.shape[2]
    tiles = cols // LANE
    width = tiles + 1
    bands = rows // SUB + 2

    lane = iota((SUB, LANE), 1)
    sub = iota((SUB, LANE), 0)

    def exists(d):
        dy, dx = DIRS[d]
        return (gy + dy >= 0) & (gy + dy < ny) & (gx + dx >= 0) & (gx + dx < nx)

    def at(d):
        dy, dx = DIRS[d]
        return {"comp": group, "gy": gy + dy, "gx": gx + dx}

    partner = {"comp": 1 - group, "gy": gy, "gx": gx}

    def copy(src, dst, d, f):
        return pltpu.make_async_remote_copy(
            src_ref=src, dst_ref=dst, send_sem=send.at[d, f], recv_sem=recv.at[OPP[d], f],
            device_id=at(d), device_id_type=MESH,
        )

    def arrival(dst, d, f):
        return pltpu.make_async_remote_copy(
            src_ref=dst, dst_ref=dst, send_sem=send.at[d, f], recv_sem=recv.at[d, f],
            device_id=at(d), device_id_type=MESH,
        )

    fields = (
        (cond_in.at[0], xf.at[0]),
        (active_in.at[0], xi.at[1]),
        (code_in.at[0], xi.at[2]),
        (head_in.at[0], xf.at[1]),
        (terrain_in, xi.at[0]),
    )
    rfrom = {-1: (0, SUB), 0: (0, rows), 1: (rows - SUB, SUB)}
    cfrom = {-1: (0, LANE), 0: (0, cols), 1: (cols - LANE, LANE)}
    rslot = {-1: (0, SUB), 0: (SUB, rows), 1: (rows + SUB, SUB)}
    cslot = {-1: (cols + LANE, LANE), 0: (0, cols), 1: (cols, LANE)}

    def cut(ref, r, c):
        return ref.at[pl.ds(r[0], r[1]), pl.ds(c[0], c[1])]

    def part(ref, d):
        return cut(ref, rfrom[DIRS[d][0]], cfrom[DIRS[d][1]])

    def slot(ref, d):
        return cut(ref, rslot[DIRS[d][0]], cslot[DIRS[d][1]])

    own = ((SUB, rows), (0, cols))

    def local_copy(src, dst, k):
        return pltpu.make_async_copy(src, dst, local.at[k])

    terrain_load = local_copy(terrain_in, cut(xi.at[0], *own), 4)
    route_loads = [local_copy(f[0], cut(f[1], *own), k) for k, f in enumerate(fields[:4])]
    water_load = local_copy(water_in.at[0], wb.at[8], 0)
    soil_load = local_copy(soil_in.at[0], mb.at[8], 1)

    barrier = pltpu.get_barrier_semaphore()
    for d in range(8):
        @pl.when(exists(d))
        def _():
            pl.semaphore_signal(barrier, inc=1, device_id=at(d), device_id_type=MESH)
    pl.semaphore_signal(barrier, inc=1, device_id=partner, device_id_type=MESH)
    greeted = 1
    for d in range(8):
        greeted = greeted + exists(d).astype(jnp.int32)

    terrain_load.start()

    @pl.when(group == 0)
    def _():
        water_load.start()
        soil_load.start()

    @pl.when(group == 1)
    def _():
        for load in route_loads:
            load.start()

    pl.semaphore_wait(barrier, greeted)

    def land_first(d):
        out = [copy(soil_in.at[0], mb.at[OPP[d]], d, 1)]
        if d < 4:
            out.insert(0, copy(water_in.at[0], wb.at[OPP[d]], d, 0))
        return out

    def land_pack(d):
        return copy(pk.at[0 if DIRS[d][1] < 0 else 1], dg.at[OPP[d] - 4], d, 0)

    def land_mean(d):
        return copy(mn.at[8], mn.at[OPP[d]], d, 2)

    def route_sends(d):
        return [copy(part(f[0], d), slot(f[1], OPP[d]), d, k) for k, f in enumerate(fields)]

    q_send = pltpu.make_async_remote_copy(
        src_ref=qb.at[0], dst_ref=qb.at[1], send_sem=hop.at[0], recv_sem=hop.at[1],
        device_id=partner, device_id_type=MESH,
    )
    back_send = pltpu.make_async_remote_copy(
        src_ref=back_tx, dst_ref=back_rx, send_sem=hop.at[2], recv_sem=hop.at[3],
        device_id=partner, device_id_type=MESH,
    )

    def over(dirs, act):
        for d in dirs:
            @pl.when(exists(d))
            def _():
                act(d)

    def start_all(copies):
        for c in copies:
            c.start()

    @pl.when(group == 0)
    def _():
        over(range(8), lambda d: start_all(land_first(d)))

    @pl.when(group == 1)
    def _():
        over(range(8), lambda d: start_all(route_sends(d)))

    k10 = iota((LANE, ccol), 1) * AGG
    j0 = iota((LANE, ccol), 0)

    for c in range(tiles):
        j = j0 + c * LANE
        gather[c * LANE : (c + 1) * LANE, :] = jnp.where(
            (j >= k10) & (j < k10 + AGG), 1.0, 0.0
        ).astype(jnp.bfloat16)

    def means(first, second):
        parts = []
        for field in (first, second):
            high, low = [], []
            for tile in field:
                a, b = halves(tile)
                high.append(a)
                low.append(b)
            parts.append(jnp.concatenate(high, axis=1))
            parts.append(jnp.concatenate(low, axis=1))
        stacked = jnp.concatenate(parts, axis=0)
        y = jnp.dot(stacked, gather[...], preferred_element_type=jnp.float32)
        i10 = iota((crow, rows), 0) * AGG
        i = iota((crow, rows), 1)
        pool = jnp.where((i >= i10) & (i < i10 + AGG), 1.0, 0.0)
        total = []
        for k in (0, 2):
            z = y[k * rows : (k + 1) * rows] + y[(k + 1) * rows : (k + 2) * rows]
            total.append(
                jnp.dot(pool, z, preferred_element_type=jnp.float32, precision=lax.Precision.HIGHEST)
                * (1.0 / (AGG * AGG))
            )
        return total

    @pl.when(group == 0)
    def _():
        water_load.wait()
        packs = [jnp.zeros((SUB, LANE), jnp.float32), jnp.zeros((SUB, LANE), jnp.float32)]
        for l in range(lev):
            mine = (lane >= 8 * l) & (lane < 8 * l + 8)
            w = wb[8, l]
            packs[0] = jnp.where(mine, pltpu.roll(w, (8 * l) % LANE, 1), packs[0])
            packs[1] = jnp.where(mine, pltpu.roll(w, (8 * l + 8) % LANE, 1), packs[1])
        pk[0] = packs[0]
        pk[1] = packs[1]
        over(range(4, 8), lambda d: land_pack(d).start())

        terrain_load.wait()
        firsts, seconds = [], []
        for c in range(tiles):
            tc = xi[0, SUB : SUB + rows, c * LANE : (c + 1) * LANE]
            firsts.append(pick(ewt, tc))
            seconds.append(pick(swt, tc))
        mean_e, mean_s = means(firsts, seconds)
        mn[8, 0] = mean_e
        mn[8, 1] = mean_s
        over(range(8), lambda d: land_mean(d).start())

        soil_load.wait()
        over(range(4), lambda d: arrival(wb.at[d], d, 0).wait_recv())
        over(range(4, 8), lambda d: arrival(dg.at[d - 4], d, 0).wait_recv())
        over(range(8), lambda d: arrival(mb.at[d], d, 1).wait_recv())

        def valid(a, b):
            r = sub + (0 if a == 0 else jnp.where(sub < 4, crow, -crow))
            r = r + gy * crow
            k = lane + (0 if b == 0 else jnp.where(lane < 64, ccol, -ccol))
            k = k + gx * ccol
            return (r >= 0) & (r < ny * crow) & (k >= 0) & (k < nx * ccol)

        ok = [[valid(a, b) for b in range(2)] for a in range(2)]
        left = lane < 64
        upper = sub < 4

        def joined(get, corner, fill):
            t = [
                [get(8), jnp.where(left, get(E), get(W))],
                [jnp.where(upper, get(S), get(N)), corner],
            ]
            return [[jnp.where(ok[a][b], t[a][b], fill) for b in range(2)] for a in range(2)]

        def corners(get):
            return jnp.where(
                upper,
                jnp.where(left, get(SE), get(SW)),
                jnp.where(left, get(NE), get(NW)),
            )

        def smooth(t):
            new = [[None, None], [None, None]]
            down = [[pltpu.roll(t[a][b], 1, 0) for b in range(2)] for a in range(2)]
            up = [[pltpu.roll(t[a][b], SUB - 1, 0) for b in range(2)] for a in range(2)]
            right = [[pltpu.roll(t[a][b], 1, 1) for b in range(2)] for a in range(2)]
            lft = [[pltpu.roll(t[a][b], LANE - 1, 1) for b in range(2)] for a in range(2)]
            for a in range(2):
                for b in range(2):
                    around = (
                        jnp.where(sub == 0, down[1 - a][b], down[a][b])
                        + jnp.where(sub == SUB - 1, up[1 - a][b], up[a][b])
                        + jnp.where(lane == 0, right[a][1 - b], right[a][b])
                        + jnp.where(lane == LANE - 1, lft[a][1 - b], lft[a][b])
                    )
                    value = t[a][b] + diffusion_rate * (around - 4.0 * t[a][b])
                    new[a][b] = jnp.where(ok[a][b], value, 0.0)
            return new

        ce = jnp.where(upper, dg[SE - 4], dg[NE - 4])
        cw = jnp.where(upper, dg[SW - 4], dg[NW - 4])
        precip = [[0.0, 0.0], [0.0, 0.0]]
        ground = None
        for l in range(lev):
            corner = jnp.where(
                left,
                pltpu.roll(ce, (LANE - 8 * l) % LANE, 1),
                pltpu.roll(cw, (2 * LANE - 8 - 8 * l) % LANE, 1),
            )
            t = joined(lambda k: wb[k, l], corner, 0.0)
            for _ in range(SWEEPS):
                t = smooth(t)
            if l == 0:
                ground = t[0][0]
            for a in range(2):
                for b in range(2):
                    precip[a][b] = precip[a][b] + lw[l] * t[a][b] * t[a][b]

        moisture = joined(lambda k: mb[k], corners(lambda k: mb[k]), 0.5)
        over(range(8), lambda d: arrival(mn.at[d], d, 2).wait_recv())
        m_e = joined(lambda k: mn[k, 0], corners(lambda k: mn[k, 0]), 1.0)
        m_s = joined(lambda k: mn[k, 1], corners(lambda k: mn[k, 1]), 1.0)
        for a in range(2):
            for b in range(2):
                m = moisture[a][b]
                excess = precip[a][b] * m * m / (m * m + half_point)
                rs = slice(a * SUB, (a + 1) * SUB)
                cs = slice(b * LANE, (b + 1) * LANE)
                qb[0, 0, rs, cs] = excess / m_e[a][b]
                qb[0, 1, rs, cs] = m / m_s[a][b]
        q_send.start()
        divisor = 1.0 + evaporation_scale * ground * ground
        over(range(8), lambda d: [c.wait_send() for c in land_first(d)])
        over(range(4, 8), lambda d: land_pack(d).wait_send())
        over(range(8), lambda d: land_mean(d).wait_send())
        q_send.wait_send()
        back_send.wait_recv()
        out_ref[0] = back_rx[...] / divisor

    R, AD, M0, M1, M2, M3, EW, HD, SO = range(9)
    WN, WS, WW, WE, AA, B0, B1, B2, B3 = range(9, 18)

    @pl.when(group == 1)
    def _():
        kk = iota((2 * ccol, LANE), 0)
        jj = iota((2 * ccol, LANE), 1)
        for c in range(tiles):
            j = jj + c * LANE
            spreadm[:, c * LANE : (c + 1) * LANE] = jnp.where(
                (j >= kk * AGG) & (j < kk * AGG + AGG), 1.0, 0.0
            ).astype(jnp.bfloat16)
        spreadm[:, cols:] = jnp.where(
            ((jj < 64) & (kk == ccol)) | ((jj >= 64) & (kk == 2 * ccol - 1)), 1.0, 0.0
        ).astype(jnp.bfloat16)

        zero = jnp.zeros((SUB, LANE), jnp.float32)
        for c in range(width):
            for edge in (0, (bands + 1) * SUB):
                for k in (R, M0, M1):
                    st[k, c, edge : edge + SUB] = zero
                for k in range(2):
                    for p in range(2):
                        ps[p, k, c, edge : edge + SUB] = zero

        def prepare(t, c):
            r = pl.ds(t * SUB if isinstance(t, int) else pl.multiple_of(t * SUB, SUB), SUB)
            o = pl.ds(
                (t + 1) * SUB if isinstance(t, int) else pl.multiple_of(t * SUB + SUB, SUB), SUB
            )

            def take(ref, k):
                a = ref[k, r, c * LANE : (c + 1) * LANE]
                if c < tiles:
                    return a
                return jnp.where(lane < 64, a, ref[k, r, (c + 1) * LANE : (c + 2) * LANE])

            row = sub + (t - 1) * SUB + gy * rows
            col = lane + c * LANE
            if c == tiles:
                col = jnp.where(lane < 64, col, lane - LANE)
            col = col + gx * cols
            ok = (row >= 0) & (row < ny * rows) & (col >= 0) & (col < nx * cols)
            active = jnp.where(ok, take(xi, 1).astype(jnp.float32), 0.0)
            code = take(xi, 2)
            keff = jnp.where(ok, take(xf, 0), 0.0) * active
            tc = take(xi, 0)
            st[R, c, o] = jnp.sqrt(keff)
            rate = drainage_rate * active
            st[AD, c, o] = rate
            for k in range(4):
                st[M0 + k, c, o] = jnp.where(code == k, rate, 0.0)
            st[EW, c, o] = active * pick(ewt, tc)
            st[HD, c, o] = active * jnp.where(ok, take(xf, 1), 0.0)
            st[SO, c, o] = pick(swt, tc)

        for load in route_loads:
            load.wait()
        terrain_load.wait()

        def inner(t, carry):
            for c in range(tiles):
                prepare(t, c)
            return carry

        lax.fori_loop(1, bands - 1, inner, 0, unroll=2)

        over(range(8), lambda d: [arrival(slot(f[1], d), d, k).wait_recv() for k, f in enumerate(fields)])

        def rim(k, carry):
            for c in range(tiles):
                prepare(k * (bands - 1), c)
            return carry

        lax.fori_loop(0, 2, rim, 0)

        def side(t, carry):
            prepare(t, tiles)
            return carry

        lax.fori_loop(0, bands, side, 0, unroll=6)

        def from_west(tile_list):
            turned = [pltpu.roll(x, 1, 1) for x in tile_list]
            return [jnp.where(lane == 0, turned[c - 1], turned[c]) for c in range(width)]

        def from_east(tile_list):
            turned = [pltpu.roll(x, LANE - 1, 1) for x in tile_list]
            return [
                jnp.where(lane == LANE - 1, turned[(c + 1) % width], turned[c])
                for c in range(width)
            ]

        def couple(t, carry):
            base = pl.multiple_of(t * SUB + SUB, SUB)
            o = pl.ds(base, SUB)
            above = pl.ds(base - 1, SUB)
            below = pl.ds(base + 1, SUB)
            r = [st[R, c, o] for c in range(width)]
            west, east = from_west(r), from_east(r)
            for c in range(width):
                wn = r[c] * st[R, c, above]
                ws = r[c] * st[R, c, below]
                ww = r[c] * west[c]
                we = r[c] * east[c]
                st[WN, c, o] = wn
                st[WS, c, o] = ws
                st[WW, c, o] = ww
                st[WE, c, o] = we
                st[AA, c, o] = (wn + ws) + (ww + we)
                st[B0, c, o] = st[M0, c, below]
                st[B1, c, o] = st[M1, c, above]
            for c, v in enumerate(from_east([st[M2, c, o] for c in range(width)])):
                st[B2, c, o] = v
            for c, v in enumerate(from_west([st[M3, c, o] for c in range(width)])):
                st[B3, c, o] = v
            return carry

        lax.fori_loop(0, bands, couple, 0, unroll=4)

        q_send.wait_recv()
        high, low = [], []
        for k in range(2):
            a, b = halves(qb[1, k])
            high.append(a)
            low.append(b)
        y = jnp.dot(
            jnp.concatenate(high + low, axis=0), spreadm[...], preferred_element_type=jnp.float32
        )
        qx[...] = y[: 4 * SUB] + y[4 * SUB :]
        for t in range(bands):
            o = slice((t + 1) * SUB, (t + 2) * SUB)
            if t == 0:
                a = b = 2 * crow - 1
            elif t == bands - 1:
                a = b = crow
            else:
                a, b = ((t - 1) * SUB) // AGG, ((t - 1) * SUB + SUB - 1) // AGG
            for c in range(width):
                cs = slice(c * LANE, (c + 1) * LANE)

                def up(k):
                    first = jnp.broadcast_to(qx[k * 16 + a : k * 16 + a + 1, cs], (SUB, LANE))
                    if a == b:
                        return first
                    second = jnp.broadcast_to(qx[k * 16 + b : k * 16 + b + 1, cs], (SUB, LANE))
                    return jnp.where(sub < b * AGG - (t - 1) * SUB, first, second)

                ps[0, 0, c, o] = st[HD, c, o] + st[EW, c, o] * up(0)
                ps[0, 1, c, o] = st[SO, c, o] * up(1)

        def substep(src, dst):
            def band(t, carry):
                base = pl.multiple_of(t * SUB + SUB, SUB)
                o = pl.ds(base, SUB)
                above = pl.ds(base - 1, SUB)
                below = pl.ds(base + 1, SUB)
                p = [ps[src, 0, c, o] for c in range(width)]
                s = [ps[src, 1, c, o] for c in range(width)]
                ss = [x * x for x in s]
                p_w, p_e = from_west(p), from_east(p)
                s_w, s_e = from_west(ss), from_east(ss)
                for c in range(width):
                    s_n = ps[src, 1, c, above]
                    s_s = ps[src, 1, c, below]
                    spread = (
                        st[WN, c, o] * ps[src, 0, c, above]
                        + st[WS, c, o] * ps[src, 0, c, below]
                        + (st[WW, c, o] * p_w[c] + st[WE, c, o] * p_e[c])
                        - st[AA, c, o] * p[c]
                    )
                    soaked = infiltration_rate * p[c] * pl.reciprocal(1.0 + s[c])
                    inflow = (
                        st[B0, c, o] * (s_s * s_s)
                        + st[B1, c, o] * (s_n * s_n)
                        + (st[B2, c, o] * s_e[c] + st[B3, c, o] * s_w[c])
                        - st[AD, c, o] * ss[c]
                    )
                    ps[dst, 0, c, o] = p[c] + (spread - soaked)
                    ps[dst, 1, c, o] = s[c] + (soaked + inflow)
                return carry

            lax.fori_loop(0, bands, band, 0, unroll=12)

        def two(k, carry):
            substep(0, 1)
            substep(1, 0)
            return carry

        lax.fori_loop(0, NSUB // 2, two, 0)

        inside = slice(2 * SUB, 2 * SUB + rows)
        mean_p, mean_st = means(
            [ps[0, 0, c, inside] for c in range(tiles)],
            [ps[0, 1, c, inside] for c in range(tiles)],
        )
        back_tx[...] = mean_st
        back_send.start()
        out_ref[0] = mean_p
        over(range(8), lambda d: [c.wait_send() for c in route_sends(d)])
        back_send.wait_send()


def per_device(ny, nx, column_water, land_soil, level_weight, excess_weight, soil_weight,
               terrain_class, surface_head, conductivity, active_mask, flow_code):
    rows, cols = terrain_class.shape
    lev = column_water.shape[1]
    crow, ccol = land_soil.shape[1:]
    wide = cols // LANE + 1
    tall = rows + 4 * SUB
    f32, i32 = jnp.float32, jnp.int32
    any_spec = pl.BlockSpec(memory_space=pltpu.HBM)
    smem = pl.BlockSpec(memory_space=pltpu.SMEM)
    return pl.pallas_call(
        functools.partial(kernel, ny, nx),
        out_shape=jax.ShapeDtypeStruct((1, crow, ccol), f32),
        in_specs=[smem] * 3 + [any_spec] * 7,
        out_specs=pl.BlockSpec(memory_space=pltpu.VMEM),
        scratch_shapes=[
            pltpu.VMEM((3, rows + 2 * SUB, cols + 2 * LANE), i32),
            pltpu.VMEM((2, rows + 2 * SUB, cols + 2 * LANE), f32),
            pltpu.VMEM((18, wide, tall, LANE), f32),
            pltpu.VMEM((2, 2, wide, tall, LANE), f32),
            pltpu.VMEM((9, lev, crow, ccol), f32),
            pltpu.VMEM((9, crow, ccol), f32),
            pltpu.VMEM((2, crow, ccol), f32),
            pltpu.VMEM((4, crow, ccol), f32),
            pltpu.VMEM((9, 2, crow, ccol), f32),
            pltpu.VMEM((2, 2, 2 * crow, 2 * ccol), f32),
            pltpu.VMEM((4 * crow, cols + LANE), f32),
            pltpu.VMEM((crow, ccol), f32),
            pltpu.VMEM((crow, ccol), f32),
            pltpu.VMEM((cols, ccol), jnp.bfloat16),
            pltpu.VMEM((2 * ccol, cols + LANE), jnp.bfloat16),
            pltpu.SemaphoreType.DMA((8, 5)),
            pltpu.SemaphoreType.DMA((8, 5)),
            pltpu.SemaphoreType.DMA((5,)),
            pltpu.SemaphoreType.DMA((4,)),
        ],
        compiler_params=pltpu.CompilerParams(
            collective_id=0, has_side_effects=True
        ),
    )(level_weight, excess_weight, soil_weight, column_water, land_soil, terrain_class,
      surface_head, conductivity, active_mask, flow_code)


def solution(mesh):
    in_specs = (
        P("comp", None, "gy", "gx"),
        P("comp", "gy", "gx"),
        P(),
        P(),
        P(),
        P("gy", "gx"),
        P("comp", "gy", "gx"),
        P("comp", "gy", "gx"),
        P("comp", "gy", "gx"),
        P("comp", "gy", "gx"),
    )
    body = functools.partial(per_device, mesh.shape["gy"], mesh.shape["gx"])
    return jax.shard_map(
        body, mesh=mesh, in_specs=in_specs, out_specs=P("comp", "gy", "gx"), check_vma=False
    )
```
